32 devices in a mesh: grp: 2 (over x), path: 8 (over z, y), state: 2 (over core).
Axes of the slice: x: 2, y: 2, z: 4, core: 2. Of those that a mesh axis runs over, the one named last changes fastest.
Arguments:
- start_states: bfloat16 [2, 2, 128, 128, 128], P(None, 'state', 'path'), may hold values from -6 to 6
- block_gates: bfloat16 [3, 2, 128, 128], replicated, may hold values from -0.5 to 0.5
- cut_ops: float32 [2, 6, 2, 2, 2], replicated, may hold values from -4 to 4
- path_bits: int32 [16, 6], P(('grp', 'path')), parts along dimension 0, may hold values from 0 to 1
- left_pick: int32 [8], replicated, may hold values from 0 to 4194303
- right_pick: int32 [8], replicated, may hold values from 0 to 4194303
Outputs:
- amp_left: float32 [16, 2, 128, 128, 128], P('grp', 'state', 'path'), parts along dimension 0
- amp_right: float32 [16, 2, 128, 128, 128], P('grp', 'state', 'path'), parts along dimension 0
The draws below stay inside these ranges and needn't reach their ends.
There are 2 independent parts, one for each index of `grp`. The reference program is written for one: setup_inputs(seed, part) draws one part's arguments, and reference() takes and returns one part's arrays. A program takes and returns all parts, laid end to end along the dimension named above; an argument that names none is the same for every part. Nothing has to cross between parts.
All inputs are finite; a program needn't handle non-finite values.
Results may differ from the reference program's by a relative error of at most 0.0085.
Values may be sent and summed in bfloat16 or wider, within the bound.
No kernel may reach another device: no remote copies, remote signals or barrier semaphores. Data moves between devices by JAX's collectives and lax.ppermute only.
A program may use at most 128 MiB of HBM per device.

```python
import math
import jax
import jax.numpy as jnp
from jax import lax

GATE_DIM = 128
BLOCKS = 3
CUT_BLOCK = 3
SEL = 8
CUTS = 6
PATHS = 8
N_STATE = 2


def plant(entries, own_key, smallest, top_value):
    longest = entries.shape.index(max(entries.shape))
    spots = []
    for shift in (0, 1):
        where = [jax.random.randint(jax.random.fold_in(own_key, axis), (), 0, length) for axis, length in enumerate(entries.shape)]
        where[longest] = (where[longest] + shift) % entries.shape[longest]
        spots.append(tuple(where))
    return entries.at[spots[0]].set(smallest).at[spots[1]].set(top_value)


def shard_levels(stream_key, extent, shards, low, top_value):
    def one(dim, parts):
        steps = jax.random.uniform(jax.random.fold_in(jax.random.fold_in(stream_key, 6), dim), (parts,), jnp.float32, low / len(shards), top_value / len(shards))
        return jnp.repeat(jnp.exp(steps), extent[dim] // parts).reshape((-1,) + (1,) * (len(extent) - dim - 1))

    factor_of = one(*shards[0])
    for cut in shards[1:]:
        factor_of = factor_of * one(*cut)
    return factor_of


def scatter_about(stream_key, dims, scale, most, split=(), kind=jnp.bfloat16):
    loudness = shard_levels(stream_key, dims, split, -0.22, 0.18) if split else 1.0
    array = jax.random.normal(stream_key, dims, jnp.float32) * scale * loudness
    return jnp.minimum(jnp.maximum(array, -most), most).astype(kind)


def setup_inputs(seed: int = 0, part: int = 0) -> dict:
    splits = jax.random.split(jax.random.key(seed), 7)
    part_splits = jax.random.split(jax.random.fold_in(splits[6], part), 7)
    return {
        "start_states": scatter_about(splits[0], (2, N_STATE, GATE_DIM, GATE_DIM, GATE_DIM), 1.0, 6.0, ((1, 2), (2, 8))),
        "block_gates": scatter_about(splits[1], (BLOCKS, 2, GATE_DIM, GATE_DIM), GATE_DIM ** -0.5, 0.5),
        "cut_ops": scatter_about(splits[2], (2, CUTS, 2, 2, 2), 2 ** -0.5, 4.0, (), jnp.float32),
        "path_bits": plant(jax.random.randint(part_splits[3], (PATHS, CUTS), 0, 2), jax.random.fold_in(part_splits[3], 1), 0, 1).astype(jnp.int32),
        "left_pick": plant(jax.random.randint(splits[4], (SEL,), 0, N_STATE * GATE_DIM ** 3), jax.random.fold_in(splits[4], 1), 0, (N_STATE * GATE_DIM ** 3) - 1).astype(jnp.int32),
        "right_pick": plant(jax.random.randint(splits[5], (SEL,), 0, N_STATE * GATE_DIM ** 3), jax.random.fold_in(splits[5], 1), 0, (N_STATE * GATE_DIM ** 3) - 1).astype(jnp.int32),
    }


def kron_cut(cut_pair, bit_row):
    result = jnp.eye(GATE_DIM // 2 ** CUT_BLOCK, dtype=jnp.float32)
    for position in reversed(range(CUT_BLOCK)):
        picked = jnp.where(bit_row[position] == 1, cut_pair[position, 1], cut_pair[position, 0])
        result = jnp.kron(result, picked)
    return result

def mixed_gate(matrix, cut_pair, bit_row):
    product = jnp.dot(matrix.astype(jnp.float32), kron_cut(cut_pair, bit_row), precision=lax.Precision.HIGHEST)
    return product.astype(jnp.bfloat16)

def apply_last(matrix, states):
    return jnp.einsum('...j,ij->...i', states.astype(jnp.float32), matrix.astype(jnp.float32)).astype(jnp.bfloat16)

def apply_middle(matrix, states):
    return jnp.einsum('txjz,ij->txiz', states.astype(jnp.float32), matrix.astype(jnp.float32)).astype(jnp.bfloat16)

def apply_top(matrix, states):
    viewed = states.reshape(GATE_DIM, 2, GATE_DIM, GATE_DIM)
    turned = jnp.einsum('iw,wuyz->iuyz', matrix.astype(jnp.float32), viewed.astype(jnp.float32))
    return turned.astype(jnp.bfloat16).reshape(N_STATE, GATE_DIM, GATE_DIM, GATE_DIM)

def reference(start_states, block_gates, cut_ops, path_bits, left_pick, right_pick):
    base_state = jnp.stack([apply_last(block_gates[0, which_half], start_states[which_half]) for which_half in range(2)])
    powers = 2 ** jnp.arange(CUT_BLOCK, dtype=jnp.int32)

    def first_variant(variant_code):
        bit_row = variant_code // powers % 2
        return jnp.stack([apply_middle(mixed_gate(block_gates[1, which_half], cut_ops[which_half, :CUT_BLOCK], bit_row), base_state[which_half]) for which_half in range(2)])
    variants = lax.map(first_variant, jnp.arange(2 ** CUT_BLOCK, dtype=jnp.int32))

    def one_path(bit_row):
        variant_code = jnp.sum(bit_row[:CUT_BLOCK] * powers).astype(jnp.int32)
        first_state = lax.dynamic_index_in_dim(variants, variant_code, 0, keepdims=False)
        finals = jnp.stack([apply_top(mixed_gate(block_gates[2, which_half], cut_ops[which_half, CUT_BLOCK:], bit_row[CUT_BLOCK:]), first_state[which_half]) for which_half in range(2)])
        left_vals = finals[0].reshape(-1)[left_pick]
        right_vals = finals[1].reshape(-1)[right_pick]
        return (finals, left_vals, right_vals)
    finals, left_vals, right_vals = lax.map(one_path, path_bits)
    norm_scale = 1.0 / math.sqrt(PATHS)
    left_flat = finals[:, 0].reshape(PATHS, -1)
    right_flat = finals[:, 1].reshape(PATHS, -1)
    amp_left = jnp.dot(right_vals.T, left_flat, preferred_element_type=jnp.float32) * norm_scale
    amp_right = jnp.dot(left_vals.T, right_flat, preferred_element_type=jnp.float32) * norm_scale
    out_shape = (SEL, N_STATE, GATE_DIM, GATE_DIM, GATE_DIM)
    return (amp_left.reshape(out_shape), amp_right.reshape(out_shape))
```

```python
import math

import jax
import jax.numpy as jnp
from jax import lax
from jax.experimental import pallas as pl
from jax.experimental.pallas import tpu as pltpu
from jax.sharding import PartitionSpec as P


F32 = jnp.float32
BF16 = jnp.bfloat16
KINDS = "FFFF"
PAD = 8


def cut_kernel(cut_pair, bit_row, dimension):
    result = jnp.eye(dimension // 2 ** bit_row.shape[0], dtype=jnp.float32)
    for position in reversed(range(bit_row.shape[0])):
        picked = jnp.where(bit_row[position] == 1, cut_pair[position, 1], cut_pair[position, 0])
        result = jnp.kron(result, picked)
    return result


def mixed_pair(gate_pair, cuts_pair, bit_row):
    dimension = gate_pair.shape[-1]
    mixed = [
        jnp.dot(
            gate_pair[which_half].astype(jnp.float32),
            cut_kernel(cuts_pair[which_half], bit_row, dimension),
            precision=lax.Precision.HIGHEST,
        )
        for which_half in range(2)
    ]
    return jnp.stack(mixed).astype(jnp.bfloat16)


def apply_last(matrices, states):
    return jnp.einsum(
        "h...j,hij->h...i", states, matrices, preferred_element_type=jnp.float32
    ).astype(jnp.bfloat16)


def apply_middle(matrices, states):
    return jnp.einsum(
        "hxjz,hij->hxiz", states, matrices, preferred_element_type=jnp.float32
    ).astype(jnp.bfloat16)


def order_rows(matrices, owners):
    dimension = matrices.shape[-1]
    split = matrices.reshape(2, 2, owners, dimension // (2 * owners), dimension)
    return jnp.transpose(split, (0, 2, 1, 3, 4)).reshape(2, dimension, dimension)


def top_block(states, matrices):
    dimension = states.shape[-1]
    shaped = states.reshape(2, 1, dimension // 2, 2, dimension, dimension)
    received = lax.all_to_all(shaped, "state", split_axis=3, concat_axis=1, tiled=True)
    columns = received.shape[-1]
    merged = received.reshape(2, dimension, dimension * columns)
    turned = jnp.einsum("hiw,hwc->hic", matrices, merged, preferred_element_type=jnp.float32)
    return turned.astype(jnp.bfloat16).reshape(2, dimension, dimension, columns)


def third_block(first_state, block_gates, cut_ops, bit_row, sections):
    matrices = mixed_pair(block_gates[2], cut_ops[:, sections:], bit_row[sections:])
    return top_block(first_state, order_rows(matrices, lax.axis_size("path")))


def run_paths(base_state, block_gates, cut_ops, path_bits, sections):

    def one_path(bit_row):
        first_state = apply_middle(
            mixed_pair(block_gates[1], cut_ops[:, :sections], bit_row[:sections]), base_state
        )
        return third_block(first_state, block_gates, cut_ops, bit_row, sections)

    return lax.map(one_path, path_bits)


def pick_direct(finals, picks, which_half, owner_index, owners):
    dimension = finals.shape[-1]
    half_block = dimension // (2 * owners)
    flattened = finals[:, which_half].reshape(finals.shape[0], dimension**3)
    top_bit = picks // dimension**3
    row_index = picks // (dimension * dimension) % dimension
    rest = picks % (dimension * dimension)
    high_row = row_index // 2
    local_row = (
        high_row // half_block * (2 * half_block) + top_bit * half_block + high_row % half_block
    )
    values = jnp.take(flattened, local_row * dimension * dimension + rest, axis=1)
    return jnp.where((row_index % 2 == owner_index)[None, :], values, jnp.zeros_like(values))


def generic_body(start_states, block_gates, cut_ops, path_bits, left_pick, right_pick):
    sections = path_bits.shape[1] // 2
    base_state = apply_last(
        block_gates[0], lax.all_gather(start_states, "path", axis=2, tiled=True)
    )[:, 0]
    finals = run_paths(base_state, block_gates, cut_ops, path_bits, sections)
    owner_index = lax.axis_index("state")
    owners = lax.axis_size("path")
    chosen = jnp.stack(
        [
            pick_direct(finals, left_pick, 0, owner_index, owners),
            pick_direct(finals, right_pick, 1, owner_index, owners),
        ],
        axis=1,
    )
    pooled = lax.all_gather(chosen, ("path", "state"), axis=0, tiled=True)
    per_device = chosen.shape[0]
    selected = chosen.shape[-1]
    pooled = pooled.reshape(-1, lax.axis_size("state"), per_device, 2, selected)
    merged = (
        jnp.sum(pooled.astype(jnp.float32), axis=1).astype(jnp.bfloat16).reshape(-1, 2, selected)
    )
    left_vals = merged[:, 0]
    right_vals = merged[:, 1]
    norm_scale = 1.0 / math.sqrt(merged.shape[0])
    dimension = finals.shape[-1]
    half_block = dimension // (2 * owners)
    left_split = left_vals.reshape(owners, per_device, selected)
    right_split = right_vals.reshape(owners, per_device, selected)
    shaped = finals.reshape(per_device, 2, 2 * owners, half_block, dimension, dimension)
    received = lax.all_to_all(shaped, ("path", "state"), split_axis=2, concat_axis=0, tiled=True)
    columns = received.shape[-1]
    parts = received.reshape(owners, 2, per_device, 2, half_block, dimension, columns)
    amp_left = (
        jnp.einsum(
            "pqj,puqkyz->jkuyz", right_split, parts[:, :, :, 0], preferred_element_type=jnp.float32
        )
        * norm_scale
    )
    amp_right = (
        jnp.einsum(
            "pqj,puqkyz->jkuyz", left_split, parts[:, :, :, 1], preferred_element_type=jnp.float32
        )
        * norm_scale
    )
    out_shape = (selected, 2 * half_block, dimension, columns)
    amp_left, amp_right = (amp_left.reshape(out_shape), amp_right.reshape(out_shape))
    return (amp_left[:, None], amp_right[:, None])


NZ, NY = 4, 2
ZSHIFTS = (1, 3, 2)


def z_take(array, shift):
    pairs = [(z * NY + y, ((z - shift) % NZ) * NY + y) for z in range(NZ) for y in range(NY)]
    return lax.ppermute(array, "path", pairs)


def y_take(array):
    return lax.ppermute(array, "path", [(i, i ^ 1) for i in range(NZ * NY)])


def x_take(array):
    return lax.ppermute(array, "grp", [(0, 1), (1, 0)])


def t_take(array):
    return lax.ppermute(array, "state", [(0, 1), (1, 0)])


def slot_paths():
    path = lax.axis_index("path")
    z, y = path // NY, path % NY
    rows = [((z + s) % NZ) for s in (0,) + ZSHIFTS]
    return jnp.stack([r * NY + y for r in rows] + [r * NY + (1 - y) for r in rows])


def kron3(factors):
    a0, a1, a2 = factors[..., 0, :, :], factors[..., 1, :, :], factors[..., 2, :, :]
    full = (
        a2[..., :, None, None, :, None, None]
        * a1[..., None, :, None, None, :, None]
        * a0[..., None, None, :, None, None, :]
    )
    return full.reshape(full.shape[:-6] + (8, 8))


def section_kernels(ops, bits):
    picked = jnp.where(
        (bits == 1)[None, :, :, None, None], ops[:, None, :, 1], ops[:, None, :, 0]
    )
    return kron3(picked)


def mix_kernels(gates, kernels):
    rows, dim = gates.shape[1:]
    split = gates.astype(F32).reshape(2, rows, dim // 8, 8)
    mixed = jnp.einsum("hnab,hvbc->hvnac", split, kernels, precision=lax.Precision.HIGHEST)
    return mixed.reshape(2, kernels.shape[1], rows, dim)


def pick_partials(base, block_gates, cut_ops, picks):
    dim = base.shape[-1]
    own_w = base.shape[1]
    path, top = lax.axis_index("path"), lax.axis_index("state")
    codes = jnp.stack([jnp.arange(8) // 2**k % 2 for k in range(3)], axis=1)
    z_at, y_at = picks % dim, picks // dim % dim
    x_at, t_at = picks // dim**2 % dim, picks // dim**3
    w_at, u_at = t_at * (dim // 2) + x_at // 2, x_at % 2
    z_hot = (z_at[:, :, None] == jnp.arange(dim)).astype(BF16)
    lines = jnp.einsum("hwuyz,hjz->hjwuy", base, z_hot, preferred_element_type=F32)
    lines = jnp.where((u_at == 1)[:, :, None, None], lines[:, :, :, 1], lines[:, :, :, 0])
    row2 = jnp.take_along_axis(block_gates[1], y_at[:, :, None], axis=1)
    row3 = jnp.take_along_axis(block_gates[2], w_at[:, :, None], axis=1)
    row2 = mix_kernels(row2, section_kernels(cut_ops[:, :3], codes)).astype(BF16).astype(F32)
    row3 = mix_kernels(row3, section_kernels(cut_ops[:, 3:], codes)).astype(BF16).astype(F32)
    row3 = lax.dynamic_slice_in_dim(row3, top * (dim // 2) + path * own_w, own_w, 3)
    part = jnp.einsum("hvjy,hjwy->hjvw", row2, lines, precision=lax.Precision.HIGHEST)
    return jnp.einsum("hjvw,hajw->hjva", part, row3, precision=lax.Precision.HIGHEST)


def pack_aux(partials, bits):
    flat = partials.reshape(8, 128)
    high = lax.reduce_precision(flat, 8, 7)
    middle = lax.reduce_precision(flat - high, 8, 7)
    low = flat - high - middle
    last = jnp.zeros((8, 128), F32).at[0, : bits.shape[0]].set(bits.astype(F32))
    return jnp.stack(
        [jnp.concatenate([high, middle]), jnp.concatenate([low, last])]
    ).astype(BF16)


def unpack_aux(tiles):
    wide = tiles.astype(F32)
    total = jnp.sum(wide[:, 0, :8] + (wide[:, 0, 8:] + wide[:, 1, :8]), axis=0)
    paths = tiles.shape[0] // 2
    bits = wide[:paths, 1, 8, :6].astype(jnp.int32)
    return total.reshape(2, -1, 8, 8), bits


def piece_kernel(counts_a, counts_b, has_prev, paths):
    n_a, n_b = len(counts_a), len(counts_b)

    def kernel(bases, *refs):
        part_a, part_b = refs[:n_a], refs[n_a : n_a + n_b]
        rest = refs[n_a + n_b :]
        if has_prev:
            rest = rest[:3] + rest[4:]
        mix3, mix2, gate2, out, stage, turned, summed = rest
        step = pl.program_id(0)
        rows = turned.shape[0]
        stride = rows + PAD
        block = part_a[0].shape[1]

        @pl.when(step < 4)
        def _():
            for which, (parts, counts) in enumerate(((part_a, counts_a), (part_b, counts_b))):
                for yp in range(0, block, 2):
                    sides = []
                    for i in range(2):
                        tiles = [
                            ref[s, yp + i] for ref, n in zip(parts, counts) for s in range(n)
                        ]
                        sides.append(jnp.concatenate(tiles, axis=0))
                    res = jnp.dot(
                        mix3[...], jnp.concatenate(sides, axis=1), preferred_element_type=F32
                    )
                    for i in range(2):
                        for y2 in range(2):
                            at = (2 * (yp + i) + y2) * stride
                            stage[at : at + rows, :] = res[
                                y2 * rows : (y2 + 1) * rows, i * 128 : (i + 1) * 128
                            ]
                first = pl.multiple_of((bases[which] + step * block) * 2, 2 * block)
                for r in range(rows):
                    turned[r, pl.ds(first, 2 * block), :] = stage[
                        pl.ds(r, 2 * block, stride=stride), :
                    ].astype(BF16)

        @pl.when(step >= 4)
        def _():
            w0 = (step - 4) * 2
            for g in range(4):
                cols = [
                    turned[pl.ds((w0 + i) * paths, paths), g * 32 : (g + 1) * 32, :].reshape(
                        paths * 32, 128
                    )
                    for i in range(2)
                ]
                mixed = jnp.dot(
                    mix2[...], jnp.concatenate(cols, axis=1), preferred_element_type=F32
                ).astype(BF16)
                summed[:, g * 32 : (g + 1) * 32, :] = mixed.reshape(-1, 32, 256)
            for jp in range(0, summed.shape[0], 2):
                res = jnp.dot(
                    gate2[...],
                    summed[jp : jp + 2].reshape(256, 256),
                    preferred_element_type=F32,
                )
                for a in range(2):
                    for i in range(2):
                        out[jp + a, i] = res[a * 128 : (a + 1) * 128, i * 128 : (i + 1) * 128]

    return kernel


def run_piece(lists, bases, mix3, mix2, gate2, prev, u, own_w, dim, selected, paths):
    block = 8
    arrays, specs, counts = [], [], []
    for entries in lists:
        counts.append([a.shape[0] for a, _ in entries])
        for a, first in entries:
            arrays.append(a)
            specs.append(
                pl.BlockSpec(
                    (a.shape[0], block, 16, 128),
                    lambda g, b, first=first: (0, first + jnp.minimum(g, 3), 0, 0),
                )
            )
    for m in (mix3, mix2, gate2):
        arrays.append(m)
        specs.append(pl.BlockSpec(m.shape, lambda g, b: (0, 0)))
    aliases = {}
    if prev is not None:
        aliases = {1 + len(arrays): 0}
        arrays.append(prev)
        specs.append(pl.BlockSpec(memory_space=pl.ANY))
    rows = own_w * paths
    return pl.pallas_call(
        piece_kernel(counts[0], counts[1], prev is not None, paths),
        grid_spec=pltpu.PrefetchScalarGridSpec(
            num_scalar_prefetch=1,
            grid=(4 + own_w // 2,),
            in_specs=specs,
            out_specs=pl.BlockSpec(
                (selected, 2, None, dim, dim),
                lambda g, b: (0, jnp.maximum(g - 4, 0), u, 0, 0),
            ),
            scratch_shapes=[
                pltpu.VMEM((2 * block * (rows + PAD), 128), F32),
                pltpu.VMEM((rows, dim, 128), BF16),
                pltpu.VMEM((selected, dim, 256), BF16),
            ],
        ),
        out_shape=jax.ShapeDtypeStruct((selected, own_w, 2, dim, dim), F32),
        input_output_aliases=aliases,
        compiler_params=pltpu.CompilerParams(dimension_semantics=("arbitrary",)),
        name=f"piece_u{u}",
    )(bases, *arrays)


def gather_piece(piece, own_t, kind, extra):
    tiles = own_t.shape[0]
    half = tiles // 2
    x = lax.axis_index("grp")
    if kind == "F":
        slab = piece if extra is None else jnp.concatenate([piece, extra])
    else:
        slab = lax.dynamic_slice_in_dim(piece, x * half, half, 0)
        if extra is not None:
            slab = jnp.concatenate([slab, extra])
    zr = [z_take(slab, s) for s in ZSHIFTS]
    yr = [y_take(s) for s in [slab] + zr]
    tz, ty = t_take(jnp.stack(zr)), t_take(jnp.stack(yr))
    near = [a[None] for a in [slab] + zr + yr]
    aux = None
    if extra is not None:
        at = slab.shape[0] - extra.shape[0]
        aux = jnp.concatenate(
            [jnp.stack([a[at:] for a in [slab] + zr + yr]), t_take(extra)[None], tz[:, at:], ty[:, at:]]
        )
    if kind == "F":
        arrays = near + [own_t[None], tz, ty]
        blocks = half // 8
        return [(a, 0) for a in arrays], [(a, blocks) for a in arrays], (0, half), aux
    xz, xy = x_take(jnp.stack([a[:half] for a in zr])), x_take(jnp.stack([a[:half] for a in yr]))
    txz, txy = t_take(xz), t_take(xy)
    own_a = lax.dynamic_slice_in_dim(own_t, x * half, half, 0)
    own_b = lax.dynamic_slice_in_dim(own_t, (1 - x) * half, half, 0)
    far = lax.dynamic_slice_in_dim(piece, (1 - x) * half, half, 0)
    list_a = near + [own_a[None], tz, ty]
    list_b = [far[None], xz, xy, own_b[None], txz, txy]
    return [(a, 0) for a in list_a], [(a, 0) for a in list_b], (x * half, (1 - x) * half), aux


def near_body(start_states, block_gates, cut_ops, path_bits, left_pick, right_pick):
    dim = start_states.shape[-1]
    own_w = start_states.shape[2] // 2
    paths = lax.axis_size("path")
    selected = left_pick.shape[0]
    path, top = lax.axis_index("path"), lax.axis_index("state")
    base = apply_last(block_gates[0], start_states[:, 0]).reshape(2, own_w, 2, dim, dim)
    pieces = jnp.transpose(
        base.reshape(2, own_w, 2, dim // 2, 2, dim), (0, 2, 3, 4, 1, 5)
    ).reshape(4, dim // 2, 2 * own_w, dim)
    own_t = t_take(pieces)
    picks = jnp.stack([left_pick, right_pick])
    aux_tiles = pack_aux(pick_partials(base, block_gates, cut_ops, picks), path_bits[0])
    gathered = []
    aux = None
    for k in range(4):
        list_a, list_b, bases, got = gather_piece(
            pieces[k], own_t[k], KINDS[k], aux_tiles if k == 1 else None
        )
        aux = got if got is not None else aux
        gathered.append((list_a, list_b, bases))
    partials, bits = unpack_aux(aux)
    powers = 2 ** jnp.arange(3)
    code0, code1 = jnp.sum(bits[:, :3] * powers, axis=1), jnp.sum(bits[:, 3:] * powers, axis=1)
    hot = (
        (code0[:, None] == jnp.arange(8))[:, :, None]
        & (code1[:, None] == jnp.arange(8))[:, None, :]
    ).astype(F32)
    values = jnp.einsum("hjab,pab->hpj", partials, hot, precision=lax.Precision.HIGHEST)
    values = values.astype(BF16).astype(F32) * (1.0 / math.sqrt(paths))
    cut2 = section_kernels(cut_ops[:, :3], bits[:, :3])
    cut3 = section_kernels(cut_ops[:, 3:], bits[:, 3:])
    own_rows = lax.dynamic_slice_in_dim(
        block_gates[2], top * (dim // 2) + path * own_w, own_w, 1
    )
    mix3 = mix_kernels(own_rows, cut3).astype(BF16).reshape(2, paths, own_w, 2, paths, own_w)
    mix3 = jnp.take(mix3, slot_paths(), axis=4)
    mix3 = jnp.where(top == 1, mix3[:, :, :, ::-1], mix3)
    mix3 = jnp.transpose(mix3, (0, 2, 1, 3, 4, 5)).reshape(2, own_w * paths, 2 * paths, own_w)
    eye2 = jnp.eye(2, dtype=BF16)
    mix3 = jnp.einsum("ab,hrsw->harsbw", eye2, mix3).reshape(
        2, 2 * own_w * paths, 2 * paths * 2 * own_w
    )
    weighted = jnp.einsum("hpj,hpab->hjapb", values[::-1], cut2, precision=lax.Precision.HIGHEST)
    mix2 = (
        weighted[:, :, None, :, :, None, :] * jnp.eye(4, dtype=F32)[None, None, :, None, None, :, None]
    ).reshape(2, selected * 32, paths * 32).astype(BF16)
    gate2 = jnp.einsum("ab,hij->haibj", eye2, block_gates[1]).reshape(2, 2 * dim, 2 * dim)
    outs = []
    for h in range(2):
        result = None
        for u in range(2):
            list_a, list_b, bases = gathered[2 * h + u]
            result = run_piece(
                [list_a, list_b],
                jnp.stack([jnp.asarray(b, jnp.int32) for b in bases]),
                mix3[h], mix2[h], gate2[h], result, u, own_w, dim, selected, paths,
            )
        outs.append(result.reshape(selected, 1, 2 * own_w, dim, dim))
    return tuple(outs)


def solution(mesh):
    in_specs = (P(None, "state", "path", None, None), P(), P(), P(("grp", "path"), None), P(), P())
    out_specs = (P("grp", "state", "path", None, None), P("grp", "state", "path", None, None))
    sizes = dict(mesh.shape)

    def body(start_states, block_gates, cut_ops, path_bits, left_pick, right_pick):
        fits = (
            sizes["path"] == NZ * NY
            and sizes["grp"] == 2
            and sizes["state"] == 2
            and start_states.shape[2:] == (16, 128, 128)
            and path_bits.shape == (1, 6)
            and left_pick.shape[0] == 8
        )
        form = near_body if fits else generic_body
        return form(start_states, block_gates, cut_ops, path_bits, left_pick, right_pick)

    return jax.shard_map(body, mesh=mesh, in_specs=in_specs, out_specs=out_specs, check_vma=False)
```

```python
import math

import jax
import jax.numpy as jnp
from jax import lax
from jax.experimental import pallas as pl
from jax.experimental.pallas import tpu as pltpu
from jax.sharding import PartitionSpec as P


F32 = jnp.float32
BF16 = jnp.bfloat16
PAD = 8


def cut_kernel(cut_pair, bit_row, dimension):
    result = jnp.eye(dimension // 2 ** bit_row.shape[0], dtype=jnp.float32)
    for position in reversed(range(bit_row.shape[0])):
        picked = jnp.where(bit_row[position] == 1, cut_pair[position, 1], cut_pair[position, 0])
        result = jnp.kron(result, picked)
    return result


def mixed_pair(gate_pair, cuts_pair, bit_row):
    dimension = gate_pair.shape[-1]
    mixed = [
        jnp.dot(
            gate_pair[which_half].astype(jnp.float32),
            cut_kernel(cuts_pair[which_half], bit_row, dimension),
            precision=lax.Precision.HIGHEST,
        )
        for which_half in range(2)
    ]
    return jnp.stack(mixed).astype(jnp.bfloat16)


def apply_last(matrices, states):
    return jnp.einsum(
        "h...j,hij->h...i", states, matrices, preferred_element_type=jnp.float32
    ).astype(jnp.bfloat16)


def apply_middle(matrices, states):
    return jnp.einsum(
        "hxjz,hij->hxiz", states, matrices, preferred_element_type=jnp.float32
    ).astype(jnp.bfloat16)


def order_rows(matrices, owners):
    dimension = matrices.shape[-1]
    split = matrices.reshape(2, 2, owners, dimension // (2 * owners), dimension)
    return jnp.transpose(split, (0, 2, 1, 3, 4)).reshape(2, dimension, dimension)


def top_block(states, matrices):
    dimension = states.shape[-1]
    shaped = states.reshape(2, 1, dimension // 2, 2, dimension, dimension)
    received = lax.all_to_all(shaped, "state", split_axis=3, concat_axis=1, tiled=True)
    columns = received.shape[-1]
    merged = received.reshape(2, dimension, dimension * columns)
    turned = jnp.einsum("hiw,hwc->hic", matrices, merged, preferred_element_type=jnp.float32)
    return turned.astype(jnp.bfloat16).reshape(2, dimension, dimension, columns)


def third_block(first_state, block_gates, cut_ops, bit_row, sections):
    matrices = mixed_pair(block_gates[2], cut_ops[:, sections:], bit_row[sections:])
    return top_block(first_state, order_rows(matrices, lax.axis_size("path")))


def run_paths(base_state, block_gates, cut_ops, path_bits, sections):

    def one_path(bit_row):
        first_state = apply_middle(
            mixed_pair(block_gates[1], cut_ops[:, :sections], bit_row[:sections]), base_state
        )
        return third_block(first_state, block_gates, cut_ops, bit_row, sections)

    return lax.map(one_path, path_bits)


def pick_direct(finals, picks, which_half, owner_index, owners):
    dimension = finals.shape[-1]
    half_block = dimension // (2 * owners)
    flattened = finals[:, which_half].reshape(finals.shape[0], dimension**3)
    top_bit = picks // dimension**3
    row_index = picks // (dimension * dimension) % dimension
    rest = picks % (dimension * dimension)
    high_row = row_index // 2
    local_row = (
        high_row // half_block * (2 * half_block) + top_bit * half_block + high_row % half_block
    )
    values = jnp.take(flattened, local_row * dimension * dimension + rest, axis=1)
    return jnp.where((row_index % 2 == owner_index)[None, :], values, jnp.zeros_like(values))


def generic_body(start_states, block_gates, cut_ops, path_bits, left_pick, right_pick):
    sections = path_bits.shape[1] // 2
    base_state = apply_last(
        block_gates[0], lax.all_gather(start_states, "path", axis=2, tiled=True)
    )[:, 0]
    finals = run_paths(base_state, block_gates, cut_ops, path_bits, sections)
    owner_index = lax.axis_index("state")
    owners = lax.axis_size("path")
    chosen = jnp.stack(
        [
            pick_direct(finals, left_pick, 0, owner_index, owners),
            pick_direct(finals, right_pick, 1, owner_index, owners),
        ],
        axis=1,
    )
    pooled = lax.all_gather(chosen, ("path", "state"), axis=0, tiled=True)
    per_device = chosen.shape[0]
    selected = chosen.shape[-1]
    pooled = pooled.reshape(-1, lax.axis_size("state"), per_device, 2, selected)
    merged = (
        jnp.sum(pooled.astype(jnp.float32), axis=1).astype(jnp.bfloat16).reshape(-1, 2, selected)
    )
    left_vals = merged[:, 0]
    right_vals = merged[:, 1]
    norm_scale = 1.0 / math.sqrt(merged.shape[0])
    dimension = finals.shape[-1]
    half_block = dimension // (2 * owners)
    left_split = left_vals.reshape(owners, per_device, selected)
    right_split = right_vals.reshape(owners, per_device, selected)
    shaped = finals.reshape(per_device, 2, 2 * owners, half_block, dimension, dimension)
    received = lax.all_to_all(shaped, ("path", "state"), split_axis=2, concat_axis=0, tiled=True)
    columns = received.shape[-1]
    parts = received.reshape(owners, 2, per_device, 2, half_block, dimension, columns)
    amp_left = (
        jnp.einsum(
            "pqj,puqkyz->jkuyz", right_split, parts[:, :, :, 0], preferred_element_type=jnp.float32
        )
        * norm_scale
    )
    amp_right = (
        jnp.einsum(
            "pqj,puqkyz->jkuyz", left_split, parts[:, :, :, 1], preferred_element_type=jnp.float32
        )
        * norm_scale
    )
    out_shape = (selected, 2 * half_block, dimension, columns)
    amp_left, amp_right = (amp_left.reshape(out_shape), amp_right.reshape(out_shape))
    return (amp_left[:, None], amp_right[:, None])


NZ, NY = 4, 2
ZSHIFTS = (1, 3, 2)
TILES = 16


def z_take(array, shift):
    pairs = [(z * NY + y, ((z - shift) % NZ) * NY + y) for z in range(NZ) for y in range(NY)]
    return lax.ppermute(array, "path", pairs)


def y_take(array):
    return lax.ppermute(array, "path", [(i, i ^ 1) for i in range(NZ * NY)])


def x_take(array):
    return lax.ppermute(array, "grp", [(0, 1), (1, 0)])


def t_take(array):
    return lax.ppermute(array, "state", [(0, 1), (1, 0)])


def slot_paths():
    path = lax.axis_index("path")
    z, y = path // NY, path % NY
    rows = [((z + s) % NZ) for s in (0,) + ZSHIFTS]
    return jnp.stack([r * NY + y for r in rows] + [r * NY + (1 - y) for r in rows])


def kron3(factors):
    a0, a1, a2 = factors[..., 0, :, :], factors[..., 1, :, :], factors[..., 2, :, :]
    full = (
        a2[..., :, None, None, :, None, None]
        * a1[..., None, :, None, None, :, None]
        * a0[..., None, None, :, None, None, :]
    )
    return full.reshape(full.shape[:-6] + (8, 8))


def section_kernels(ops, bits):
    picked = jnp.where(
        (bits == 1)[None, :, :, None, None], ops[:, None, :, 1], ops[:, None, :, 0]
    )
    return kron3(picked)


def mix_kernels(gates, kernels):
    rows, dim = gates.shape[1:]
    split = gates.astype(F32).reshape(2, rows, dim // 8, 8)
    mixed = jnp.einsum("hnab,hvbc->hvnac", split, kernels, precision=lax.Precision.HIGHEST)
    return mixed.reshape(2, kernels.shape[1], rows, dim)


def pick_partials(base, second, block_gates, cut_ops, picks):
    pairs, rows, dim = base[0][0].shape
    own_w = rows // 2
    path, top = lax.axis_index("path"), lax.axis_index("state")
    codes = jnp.stack([jnp.arange(8) // 2**k % 2 for k in range(3)], axis=1)
    z_at, y_at = picks % dim, picks // dim % dim
    x_at, t_at = picks // dim**2 % dim, picks // dim**3
    w_at = t_at * (dim // 2) + x_at // 2
    z_hot = (z_at[:, :, None] == jnp.arange(dim)).astype(BF16)
    lines = jnp.stack(
        [
            sum(
                jnp.einsum(
                    "yrz,jz->jyr", base[h][s],
                    jnp.where((second[h] == s)[:, None], z_hot[h], 0), preferred_element_type=F32,
                )
                for s in range(2)
            )
            for h in range(2)
        ]
    ).reshape(2, -1, pairs * 2, own_w)
    row2 = jnp.take_along_axis(block_gates[1], y_at[:, :, None], axis=1)
    row3 = jnp.take_along_axis(block_gates[2], w_at[:, :, None], axis=1)
    row2 = mix_kernels(row2, section_kernels(cut_ops[:, :3], codes))
    row3 = mix_kernels(row3, section_kernels(cut_ops[:, 3:], codes))
    row2 = lax.reduce_precision(row2, 8, 7)
    row3 = lax.reduce_precision(row3, 8, 7)
    row3 = lax.dynamic_slice_in_dim(row3, top * (dim // 2) + path * own_w, own_w, 3)
    part = jnp.einsum("hvjy,hjyw->hjvw", row2, lines, precision=lax.Precision.HIGHEST)
    return jnp.einsum("hjvw,hajw->hjva", part, row3, precision=lax.Precision.HIGHEST)


def pack_aux(partials, bits):
    flat = partials.reshape(8, 128)
    high = lax.reduce_precision(flat, 8, 7)
    middle = lax.reduce_precision(flat - high, 8, 7)
    low = flat - high - middle
    last = jnp.broadcast_to(jnp.pad(bits.astype(F32), (0, 128 - bits.shape[0])), (8, 128))
    return jnp.stack(
        [jnp.concatenate([high, middle]), jnp.concatenate([low, last])]
    ).astype(BF16)


def prepare(start_states, gate, x, own_w, dim):
    pad = dim + PAD

    def kernel(x_ref, states, gates, o00, o01, o10, o11, stage):
        outs = ((o00, o01), (o10, o11))
        for h in range(2):
            for row in range(2 * own_w):
                stage[row * pad : row * pad + dim, :] = lax.dot_general(
                    states[h, row], gates[h], (((1,), (1,)), ((), ())),
                    preferred_element_type=F32,
                )
            for s in range(2):
                u = s if h else s + x_ref[0] - 2 * s * x_ref[0]
                for yp in range(dim // 2):
                    tile = [
                        stage[pl.ds(u * pad + 2 * yp + i, own_w, stride=2 * pad), :]
                        for i in range(2)
                    ]
                    outs[h][s][yp] = jnp.concatenate(tile, axis=0).astype(BF16)

    shape = jax.ShapeDtypeStruct((dim // 2, 2 * own_w, dim), BF16)
    vmem = pl.BlockSpec(memory_space=pltpu.VMEM)
    o = pl.pallas_call(
        kernel,
        in_specs=[pl.BlockSpec(memory_space=pltpu.SMEM), vmem, vmem],
        out_specs=[vmem] * 4,
        out_shape=[shape] * 4,
        scratch_shapes=[pltpu.VMEM((2 * own_w * pad, dim), F32)],
        name="prepare",
    )(x, start_states, gate)
    return ((o[0], o[1]), (o[2], o[3]))


def set_up(ops, gate_rows, aux, own_w, selected, paths, cuts):
    half_cuts = cuts // 2
    scale = 1.0 / math.sqrt(paths)
    n_aux = len(aux)
    counts = [a.shape[0] for a in aux]
    wide = 2 * paths * 2 * own_w

    def kernel(ops_ref, rows_ref, *refs):
        parts = refs[:n_aux]
        mix3, mix2 = refs[n_aux:]
        tiles = [ref[s].astype(F32) for ref, n in zip(parts, counts) for s in range(n)]
        total = sum(t[0, :8] + (t[0, 8:] + t[1, :8]) for t in tiles)
        lane = lax.broadcasted_iota(jnp.int32, (own_w, wide), 1)
        lane_r = lax.broadcasted_iota(jnp.int32, (32, paths * 32), 1)
        row_r = lax.broadcasted_iota(jnp.int32, (32, paths * 32), 0)
        lane_t = lax.broadcasted_iota(jnp.int32, (8, 128), 1)
        lane_8 = lax.broadcasted_iota(jnp.int32, (8, paths * 32), 1)
        same = (lane_r // 8) % 4 == row_r // 8

        def entry(h, k, bit, a, b):
            at = ((h * cuts + k) * 2) * 4 + a * 2 + b
            return jnp.where(bit > 0.5, ops_ref[at + 4], ops_ref[at])

        picked = [jnp.zeros((8, paths * 32), F32) for _ in range(2)]
        cut = [jnp.zeros((32, paths * 32), F32) for _ in range(2)]
        for p in range(paths):
            bits = [tiles[p][1, 8:, k : k + 1] for k in range(cuts)]
            code = sum(
                b * float(2 ** (k % half_cuts) * (8 if k < half_cuts else 1))
                for k, b in enumerate(bits)
            ).astype(jnp.int32)
            for par in range(2):
                value = jnp.sum(
                    jnp.where(lane_t == code + 64 * par, total, 0.0), axis=1, keepdims=True
                )
                picked[par] = jnp.where(lane_8 // 32 == p, value, picked[par])
            for h in range(2):
                rows = rows_ref[h]
                for k in range(half_cuts):
                    bit = bits[half_cuts + k]
                    e = [[entry(h, half_cuts + k, bit, a, b) for b in range(2)] for a in range(2)]
                    set_ = (lane >> k) & 1 == 1
                    other = jnp.where(
                        set_, pltpu.roll(rows, 2**k, 1), pltpu.roll(rows, wide - 2**k, 1)
                    )
                    rows = rows * jnp.where(set_, e[1][1], e[0][0]) + other * jnp.where(
                        set_, e[0][1], e[1][0]
                    )
                for y2 in range(2):
                    at = (y2 * paths + p) * own_w
                    mix3[h, at : at + own_w, :] = jnp.where(
                        (lane // own_w) % 2 == y2, rows, 0.0
                    )
                factor = jnp.where(same & (lane_r // 32 == p), 1.0, 0.0)
                for k in range(half_cuts):
                    bit = bits[k][:1]
                    e = [[entry(h, k, bit, a, b) for b in range(2)] for a in range(2)]
                    factor = factor * jnp.where(
                        (row_r >> k) & 1 == 1,
                        jnp.where((lane_r >> k) & 1 == 1, e[1][1], e[1][0]),
                        jnp.where((lane_r >> k) & 1 == 1, e[0][1], e[0][0]),
                    )
                cut[h] = cut[h] + factor
        for h in range(2):
            for j in range(selected):
                row = (1 - h) * (selected // 2) + j // 2
                value = picked[j % 2][row : row + 1].astype(BF16).astype(F32) * scale
                mix2[h, j * 32 : (j + 1) * 32, :] = (cut[h] * value).astype(BF16)

    vmem = pl.BlockSpec(memory_space=pltpu.VMEM)
    specs = [pl.BlockSpec(memory_space=pltpu.SMEM), pl.BlockSpec(gate_rows.shape, lambda g: (0, 0, 0))]
    for a in aux:
        last = a.shape[1] // 2 - 1
        specs.append(
            pl.BlockSpec((a.shape[0], 2) + a.shape[2:], lambda g, last=last: (0, last, 0, 0))
        )
    shapes = [
        jax.ShapeDtypeStruct((2, 2 * own_w * paths, wide), F32),
        jax.ShapeDtypeStruct((2, selected * 32, paths * 32), BF16),
    ]
    return pl.pallas_call(
        kernel,
        grid=(1,),
        in_specs=specs,
        out_specs=[pl.BlockSpec(s.shape, lambda g: (0, 0, 0)) for s in shapes],
        out_shape=shapes,
        name="set_up",
    )(ops, gate_rows, *aux)


def piece_kernel(counts, has_prev, paths, own_w):
    n = len(counts)

    def kernel(bases, *refs):
        parts, rest = refs[:n], refs[n:]
        if has_prev:
            rest = rest[:3] + rest[4:]
        mix3, mix2, gate2, out, stage, turned, summed = rest
        step = pl.program_id(0)
        rows = turned.shape[0]
        stride = rows + PAD
        block = parts[0].shape[1]

        @pl.when(step < 4)
        def _():
            weights = mix3[...].astype(BF16)
            for yp in range(0, block, 2):
                sides = []
                for i in range(2):
                    tiles = [ref[s, yp + i] for ref, c in zip(parts, counts) for s in range(c)]
                    sides.append(jnp.concatenate(tiles, axis=0))
                res = jnp.dot(weights, jnp.concatenate(sides, axis=1), preferred_element_type=F32)
                for i in range(2):
                    for y2 in range(2):
                        at = (2 * (yp + i) + y2) * stride
                        stage[at : at + rows, :] = res[
                            y2 * rows : (y2 + 1) * rows, i * 128 : (i + 1) * 128
                        ]
            first = pl.multiple_of(step * 2 * block, 2 * block)
            for p in range(paths):
                for w in range(own_w):
                    turned[w * paths + p, pl.ds(first, 2 * block), :] = stage[
                        pl.ds(p * own_w + w, 2 * block, stride=stride), :
                    ].astype(BF16)

        @pl.when(step >= 4)
        def _():
            w0 = (step - 4) * 2
            for g in range(4):
                cols = [
                    turned[pl.ds((w0 + i) * paths, paths), g * 32 : (g + 1) * 32, :].reshape(
                        paths * 32, 128
                    )
                    for i in range(2)
                ]
                mixed = jnp.dot(
                    mix2[...], jnp.concatenate(cols, axis=1), preferred_element_type=F32
                ).astype(BF16)
                summed[:, g * 32 : (g + 1) * 32, :] = mixed.reshape(-1, 32, 256)
            for jp in range(0, summed.shape[0], 2):
                res = jnp.dot(
                    gate2[...],
                    summed[jp : jp + 2].reshape(256, 256),
                    preferred_element_type=F32,
                )
                for a in range(2):
                    for i in range(2):
                        out[jp + a, i] = res[a * 128 : (a + 1) * 128, i * 128 : (i + 1) * 128]

    return kernel


def run_piece(entries, h, u, mix3, mix2, gate2, prev, own_w, dim, selected, paths):
    arrays, specs, counts = [], [], []
    for a in entries:
        counts.append(a.shape[0])
        arrays.append(a)
        specs.append(
            pl.BlockSpec(
                (a.shape[0], TILES) + a.shape[2:], lambda g, b: (0, jnp.minimum(g, 3), 0, 0)
            )
        )
    for m in (mix3, mix2, gate2):
        arrays.append(m)
        specs.append(pl.BlockSpec((None,) + m.shape[1:], lambda g, b: (h, 0, 0)))
    aliases = {}
    if prev is not None:
        aliases = {1 + len(arrays): 0}
        arrays.append(prev)
        specs.append(pl.BlockSpec(memory_space=pl.ANY))
    rows = own_w * paths
    return pl.pallas_call(
        piece_kernel(counts, prev is not None, paths, own_w),
        grid_spec=pltpu.PrefetchScalarGridSpec(
            num_scalar_prefetch=1,
            grid=(4 + own_w // 2,),
            in_specs=specs,
            out_specs=pl.BlockSpec(
                (selected, 2, None, dim, dim),
                lambda g, b: (0, jnp.maximum(g - 4, 0), b[0], 0, 0),
            ),
            scratch_shapes=[
                pltpu.VMEM((2 * TILES * (rows + PAD), 128), F32),
                pltpu.VMEM((rows, dim, 128), BF16),
                pltpu.VMEM((selected, dim, 256), BF16),
            ],
        ),
        out_shape=jax.ShapeDtypeStruct((selected, own_w, 2, dim, dim), F32),
        input_output_aliases=aliases,
        compiler_params=pltpu.CompilerParams(dimension_semantics=("arbitrary",)),
    )(jnp.asarray(u, jnp.int32).reshape(1), *arrays)


def gate_rows_in_slots(gates, own_w, dim):
    path, top = lax.axis_index("path"), lax.axis_index("state")
    own = lax.dynamic_slice_in_dim(gates, top * (dim // 2) + path * own_w, own_w, 1)
    paths = slot_paths()
    tops = jnp.stack([top, 1 - top])
    starts = tops[:, None] * (dim // 2) + paths[None, :] * own_w
    columns = starts[:, :, None, None] + jnp.arange(own_w) + jnp.zeros((2, 1), jnp.int32)
    hot = (columns.reshape(1, -1) == jnp.arange(dim)[:, None]).astype(BF16)
    return jnp.einsum("hwc,cs->hws", own, hot, preferred_element_type=F32)


def near_body(start_states, block_gates, cut_ops, path_bits, left_pick, right_pick):
    dim = start_states.shape[-1]
    own_w = start_states.shape[2] // 2
    paths = lax.axis_size("path")
    selected = left_pick.shape[0]
    cuts = path_bits.shape[1]
    x = lax.axis_index("grp")
    base = prepare(start_states[:, 0], block_gates[0], x.astype(jnp.int32).reshape(1), own_w, dim)
    picks = jnp.stack([left_pick, right_pick])
    u_at = picks // dim**2 % 2
    second = jnp.stack([(u_at[0] + x) % 2, u_at[1]])

    z_l = [z_take(base[0][0], s) for s in ZSHIFTS]
    y_l = [y_take(a) for a in [base[0][0]] + z_l]
    own = [[t_take(base[h][s]) for s in range(2)] for h in range(2)]
    zs_l, ys_l = jnp.stack(z_l), jnp.stack(y_l)
    tz_l, ty_l = t_take(zs_l), t_take(ys_l)
    x_z, x_y = x_take(zs_l), x_take(ys_l)
    tx_z, tx_y = t_take(x_z), t_take(x_y)

    partials = pick_partials(base, second, block_gates, cut_ops, picks)
    aux = pack_aux(partials, path_bits[0])
    first = jnp.concatenate([base[1][0], aux])
    f = []
    for piece in (first, base[1][1]):
        z_f = [z_take(piece, r) for r in ZSHIFTS]
        y_f = [y_take(a) for a in [piece] + z_f]
        tz_f, ty_f = t_take(jnp.stack(z_f)), t_take(jnp.stack(y_f))
        f.append(([a[None] for a in [piece] + z_f + y_f], tz_f, ty_f))
    own_aux = t_take(aux)

    gate_rows = gate_rows_in_slots(block_gates[2], own_w, dim)
    eye2 = jnp.eye(2, dtype=BF16)
    gate2 = jnp.einsum("ab,hij->haibj", eye2, block_gates[1]).reshape(2, 2 * dim, 2 * dim)
    mix3, mix2 = set_up(
        cut_ops.reshape(-1), gate_rows, f[0][0] + [own_aux[None], f[0][1], f[0][2]],
        own_w, selected, paths, cuts,
    )
    sizes = (own_w, dim, selected, paths)
    near = [a[None] for a in [base[0][0]] + z_l + y_l]
    k1 = run_piece(near + [own[0][0][None], tz_l, ty_l], 0, x, mix3, mix2, gate2, None, *sizes)
    k3 = run_piece(
        f[0][0] + [own[1][0][None], f[0][1], f[0][2]], 1, 0, mix3, mix2, gate2, None, *sizes
    )
    k2 = run_piece(
        [base[0][1][None], x_z, x_y, own[0][1][None], tx_z, tx_y],
        0, 1 - x, mix3, mix2, gate2, k1, *sizes,
    )
    k4 = run_piece(
        f[1][0] + [own[1][1][None], f[1][1], f[1][2]], 1, 1, mix3, mix2, gate2, k3, *sizes
    )
    shape = (selected, 1, 2 * own_w, dim, dim)
    return k2.reshape(shape), k4.reshape(shape)


def solution(mesh):
    in_specs = (P(None, "state", "path", None, None), P(), P(), P(("grp", "path"), None), P(), P())
    out_specs = (P("grp", "state", "path", None, None), P("grp", "state", "path", None, None))
    sizes = dict(mesh.shape)

    def fits(start_states, path_bits, left_pick):
        return (
            sizes["path"] == NZ * NY
            and sizes["grp"] == 2
            and sizes["state"] == 2
            and start_states.shape[2:] == (128, 128, 128)
            and path_bits.shape[1] == 6
            and left_pick.shape[0] == 8
        )

    def whole(start_states, block_gates, cut_ops, path_bits, left_pick, right_pick):
        near = fits(start_states, path_bits, left_pick)

        def body(*args):
            return (near_body if near else generic_body)(*args)

        step = jax.shard_map(
            body, mesh=mesh, in_specs=in_specs, out_specs=out_specs, check_vma=False
        )
        return step(start_states, block_gates, cut_ops, path_bits, left_pick, right_pick)

    return whole
```
